32 devices in a mesh: fsdp: 4 (over z), ep: 8 (over y, x, core).
Axes of the slice: x: 2, y: 2, z: 4, core: 2. Of those that a mesh axis runs over, the one named last changes fastest.
Arguments:
- layer_in: bfloat16 [65536, 1024], P(('fsdp', 'ep'))
- out_grad: bfloat16 [65536, 1024], P(('fsdp', 'ep'))
- expert_ids: int32 [65536, 8], P(('fsdp', 'ep'))
- gate_vals: float32 [65536, 8], P(('fsdp', 'ep'))
- w_one: bfloat16 [32, 1024, 512], P('ep', 'fsdp')
- w_two: bfloat16 [32, 512, 1024], P('ep', None, 'fsdp')
- w_three: bfloat16 [32, 1024, 512], P('ep', 'fsdp')
Outputs:
- output 1: bfloat16 [65536, 1024], P(('fsdp', 'ep'))
- output 2: float32 [65536, 8], P(('fsdp', 'ep'))
- output 3: float32 [32, 1024, 512], P('ep', 'fsdp')
- output 4: float32 [32, 512, 1024], P('ep', None, 'fsdp')
- output 5: float32 [32, 1024, 512], P('ep', 'fsdp')
All inputs are finite; a program needn't handle non-finite values.
Results may differ from the reference program's by a relative error of at most 0.0103656.
Values are sent between devices in bfloat16 or wider.
A program may use at most 1 GiB of HBM per device.

```python
import jax
import jax.numpy as jnp
from jax import lax

HIDDEN = 1024
EXPERT_FF = 512
EXPERTS = 32
TOP_K = 8
TOKENS_DEV = 2048
SHARDS = 32
CAPACITY = 640
TOKENS = SHARDS * TOKENS_DEV


def draw_routing(key):
    key_bias, key_hot, key_noise = jax.random.split(key, 3)
    noise_range = 65536
    spread = noise_range * TOP_K // (2 * EXPERTS)
    bias = jax.random.randint(key_bias, (EXPERTS,), 0, spread + 1)
    hot_expert = jax.random.randint(key_hot, (), 0, EXPERTS)
    expert_pos = jnp.arange(EXPERTS, dtype=jnp.int32)
    bias = bias + jnp.where(expert_pos == hot_expert, noise_range // 4, 0)
    noise = jax.random.randint(key_noise, (TOKENS, EXPERTS), 0, noise_range)
    scores = (noise + bias[None, :]) * EXPERTS + expert_pos[None, :]
    return lax.top_k(scores, TOP_K)[1].astype(jnp.int32)


def setup_inputs(seed: int = 0) -> dict:
    keys = jax.random.split(jax.random.key(seed), 7)
    layer_in = jax.random.normal(keys[0], (TOKENS, HIDDEN), jnp.float32).astype(jnp.bfloat16)
    out_grad = jax.random.normal(keys[1], (TOKENS, HIDDEN), jnp.float32).astype(jnp.bfloat16)
    expert_ids = draw_routing(keys[2])
    gate_vals = jax.random.uniform(keys[3], (TOKENS, TOP_K), jnp.float32, 0.25, 1.0)
    w_one = (jax.random.normal(keys[4], (EXPERTS, HIDDEN, EXPERT_FF), jnp.float32) * HIDDEN ** -0.5).astype(jnp.bfloat16)
    w_two = (jax.random.normal(keys[5], (EXPERTS, EXPERT_FF, HIDDEN), jnp.float32) * EXPERT_FF ** -0.5).astype(jnp.bfloat16)
    w_three = (jax.random.normal(keys[6], (EXPERTS, HIDDEN, EXPERT_FF), jnp.float32) * HIDDEN ** -0.5).astype(jnp.bfloat16)
    return {"layer_in": layer_in, "out_grad": out_grad, "expert_ids": expert_ids, "gate_vals": gate_vals, "w_one": w_one, "w_two": w_two, "w_three": w_three}


def reference(layer_in, out_grad, expert_ids, gate_vals, w_one, w_two, w_three):
    w_one_full = w_one.astype(jnp.float32)
    w_two_full = w_two.astype(jnp.float32)
    w_three_full = w_three.astype(jnp.float32)
    places = EXPERTS * CAPACITY
    expert_pos = jnp.arange(EXPERTS, dtype=jnp.int32)
    token_of = jnp.arange(TOKENS_DEV * TOP_K, dtype=jnp.int32) // TOP_K

    def shard_step(carry, shard):
        x_loc, dy_loc, ids_loc, gates_loc = shard
        flat_ids = ids_loc.reshape(-1)
        onehot = (flat_ids[:, None] == expert_pos[None, :]).astype(jnp.int32)
        before = jnp.cumsum(onehot, axis=0) - onehot
        position = jnp.sum(before * onehot, axis=1)
        slot_of = jnp.where(position < CAPACITY, flat_ids * CAPACITY + position, places)
        source = jnp.full((places,), TOKENS_DEV, jnp.int32).at[slot_of].set(token_of, mode="drop")
        slot_gate = jnp.zeros((places,), jnp.float32).at[slot_of].set(gates_loc.reshape(-1), mode="drop")
        x_buf = jnp.take(x_loc, source, axis=0, mode="fill", fill_value=0).reshape(EXPERTS, CAPACITY, HIDDEN).astype(jnp.float32)
        dy_buf = jnp.take(dy_loc, source, axis=0, mode="fill", fill_value=0).reshape(EXPERTS, CAPACITY, HIDDEN).astype(jnp.float32)
        h_one = jnp.einsum("ecd,edf->ecf", x_buf, w_one_full)
        h_three = jnp.einsum("ecd,edf->ecf", x_buf, w_three_full)
        sig_one = jax.nn.sigmoid(h_one)
        silu_one = h_one * sig_one
        act_bf = (silu_one * h_three).astype(jnp.bfloat16).astype(jnp.float32)
        y_buf = jnp.einsum("ecf,efd->ecd", act_bf, w_two_full)
        gate_buf = jnp.sum(dy_buf * y_buf, axis=-1)
        g_buf = (slot_gate.reshape(EXPERTS, CAPACITY, 1) * dy_buf).astype(jnp.bfloat16).astype(jnp.float32)
        d_act = jnp.einsum("ecd,efd->ecf", g_buf, w_two_full)
        dh_one = (d_act * h_three * sig_one * (1.0 + h_one * (1.0 - sig_one))).astype(jnp.bfloat16).astype(jnp.float32)
        dh_three = (d_act * silu_one).astype(jnp.bfloat16).astype(jnp.float32)
        dx_buf = (jnp.einsum("ecf,edf->ecd", dh_one, w_one_full) + jnp.einsum("ecf,edf->ecd", dh_three, w_three_full)).astype(jnp.bfloat16)
        dx_pick = jnp.take(dx_buf.reshape(places, HIDDEN), slot_of, axis=0, mode="fill", fill_value=0).reshape(TOKENS_DEV, TOP_K, HIDDEN)
        dx_tok = jnp.sum(dx_pick.astype(jnp.float32), axis=1).astype(jnp.bfloat16)
        gate_tok = jnp.take(gate_buf.reshape(places), slot_of, axis=0, mode="fill", fill_value=0).reshape(TOKENS_DEV, TOP_K)
        acc_one, acc_two, acc_three = carry
        acc_one = acc_one + jnp.einsum("ecd,ecf->edf", x_buf, dh_one)
        acc_two = acc_two + jnp.einsum("ecf,ecd->efd", act_bf, g_buf)
        acc_three = acc_three + jnp.einsum("ecd,ecf->edf", x_buf, dh_three)
        return (acc_one, acc_two, acc_three), (dx_tok, gate_tok)

    init = (jnp.zeros((EXPERTS, HIDDEN, EXPERT_FF), jnp.float32), jnp.zeros((EXPERTS, EXPERT_FF, HIDDEN), jnp.float32), jnp.zeros((EXPERTS, HIDDEN, EXPERT_FF), jnp.float32))
    shards = (layer_in.reshape(SHARDS, TOKENS_DEV, HIDDEN), out_grad.reshape(SHARDS, TOKENS_DEV, HIDDEN), expert_ids.reshape(SHARDS, TOKENS_DEV, TOP_K), gate_vals.reshape(SHARDS, TOKENS_DEV, TOP_K))
    (grad_one, grad_two, grad_three), (in_grad, gate_grad) = lax.scan(shard_step, init, shards)
    return in_grad.reshape(TOKENS, HIDDEN), gate_grad.reshape(TOKENS, TOP_K), grad_one, grad_two, grad_three
```

```python
import functools

import jax
import jax.numpy as jnp
from jax import lax
from jax.experimental import pallas as pl
from jax.experimental.pallas import tpu as pltpu
from jax.sharding import PartitionSpec as P

TILE = 256
ALIGN = 16
WIN = TILE + ALIGN
BACK = TILE - ALIGN
F32 = jnp.float32
BF16 = jnp.bfloat16


def capacity_of(tok_dev, top_k, experts):
    return max(8, ((tok_dev * top_k * 5) // (4 * experts) + 7) // 8 * 8)


def dot_nn(a, b):
    return lax.dot_general(a, b, (((1,), (0,)), ((), ())), preferred_element_type=F32)


def dot_nt(a, b):
    return lax.dot_general(a, b, (((1,), (1,)), ((), ())), preferred_element_type=F32)


def dot_tn(a, b):
    return lax.dot_general(a, b, (((0,), (0,)), ((), ())), preferred_element_type=F32)


def expert_kernel(first, capacity, rows_blk, starts, pos, gate, xa, xb, ya, yb, w_up, w_down, *rest):
    if first:
        dx, dgate, g_up, g_down = rest[:4]
        scratch = rest[4:]
    else:
        acc_up, acc_down, dx, dgate, g_up, g_down = rest[:6]
        scratch = rest[6:]
    xbuf, ybuf, xs, us, gs, dgs, dhs, acts, sems = scratch
    step = pl.program_id(0)
    tok = xbuf.shape[1]
    hidden = xbuf.shape[2]
    ff = acts.shape[1]
    tiles = tok // TILE

    def copies(src):
        x_ref, y_ref = ((xa, ya), (xb, yb))[src]
        return (pltpu.make_async_copy(x_ref, xbuf.at[src], sems.at[src, 0]),
                pltpu.make_async_copy(y_ref, ybuf.at[src], sems.at[src, 1]))

    @pl.when(step == 0)
    def _():
        for src in range(2):
            for cp in copies(src):
                cp.start()

    if first:
        g_up[...] = jnp.zeros_like(g_up)
        g_down[...] = jnp.zeros_like(g_down)
    else:
        g_up[...] = acc_up[...]
        g_down[...] = acc_down[...]

    @pl.when(step == 0)
    def _():
        for src in range(2):
            for cp in copies(src):
                cp.wait()

    slot_iota = lax.broadcasted_iota(jnp.int32, (WIN, TILE), 0)

    def source_body(src, carry):
        xs[0:capacity, :] = jnp.zeros((capacity, hidden), BF16)
        us[0:capacity, :] = jnp.zeros((capacity, hidden), BF16)
        gs[0:capacity, :] = jnp.zeros((capacity, 128), F32)

        def pick(i, carry):
            start = pl.multiple_of(starts[step, src, i], ALIGN)
            pos_row = pos[0, src, pl.ds(i, 1), :]
            gate_row = gate[0, src, pl.ds(i, 1), :]
            hit = (slot_iota + start) == pos_row
            onehot = jnp.where(hit, 1.0, 0.0).astype(BF16)
            tok0 = pl.multiple_of(i * TILE, TILE)
            for buf, rows in ((xbuf, xs), (ybuf, us)):
                for c in range(0, hidden, 256):
                    got = dot_nn(onehot, buf[src, pl.ds(tok0, TILE), c:c + 256]).astype(BF16)
                    rows[pl.ds(start, ALIGN), c:c + 256] = rows[pl.ds(start, ALIGN), c:c + 256] + got[:ALIGN]
                    rows[pl.ds(start + ALIGN, TILE), c:c + 256] = got[ALIGN:]
            got_gate = jnp.sum(jnp.where(hit, gate_row, 0.0), axis=1, keepdims=True)
            got_gate = jnp.broadcast_to(got_gate, (WIN, 128))
            gs[pl.ds(start, ALIGN), :] = gs[pl.ds(start, ALIGN), :] + got_gate[:ALIGN]
            gs[pl.ds(start + ALIGN, TILE), :] = got_gate[ALIGN:]
            return carry

        lax.fori_loop(0, tiles, pick, 0)

        def rows_body(b, carry):
            r0 = pl.multiple_of(b * rows_blk, rows_blk)
            rows = pl.ds(r0, rows_blk)
            up = w_up[...].reshape(hidden, 2 * ff)
            down = w_down[...].reshape(hidden, ff)
            h = dot_nn(xs[rows, :], up)
            h_one = h[:, :ff]
            h_three = h[:, ff:]
            sig = jax.nn.sigmoid(h_one)
            silu = h_one * sig
            act = (silu * h_three).astype(BF16)
            acts[rows, :] = act
            u = us[rows, :].astype(F32)
            y = dot_nt(act, down)
            dg = jnp.sum(u * y, axis=1, keepdims=True)
            dgs[rows, :] = jnp.broadcast_to(dg, (rows_blk, 128))
            g = (gs[rows, 0:1] * u).astype(BF16)
            us[rows, :] = g
            da = dot_nn(g, down)
            dh_one = (da * h_three * sig * (1.0 + h_one * (1.0 - sig))).astype(BF16)
            dh_three = (da * silu).astype(BF16)
            dhs[rows, 0:ff] = dh_one
            dhs[rows, ff:2 * ff] = dh_three
            dx[0, src, rows, :] = dot_nt(dhs[rows, :], up).astype(BF16)
            return carry

        lax.fori_loop(0, capacity // rows_blk, rows_body, 0)

        quarter = g_up.shape[2]
        for z in range(g_up.shape[0]):
            cols = slice(z * quarter, (z + 1) * quarter)
            g_up[z, 0] += dot_tn(xs[0:capacity, cols], dhs[...])
            g_down[z, 0] += dot_tn(us[0:capacity, cols], acts[...])

        def give(i, carry):
            start = pl.multiple_of(starts[step, src, i], ALIGN)
            hit = (slot_iota + start) == pos[0, src, pl.ds(i, 1), :]
            val = dgs[pl.ds(start, WIN), :]
            val = jnp.concatenate([val, val], axis=1)
            dgate[0, src, pl.ds(i, 1), :] = jnp.sum(jnp.where(hit, val, 0.0), axis=0, keepdims=True)
            return carry

        lax.fori_loop(0, tiles, give, 0)
        return carry

    lax.fori_loop(0, 2, source_body, 0)


def run_experts(starts, pos, gate, xa, xb, ya, yb, w_up, w_down, acc):
    n_exp, _, tiles, _ = pos.shape
    tok, hidden = xa.shape
    parts, _, quarter, two_ff = w_up.shape
    ff = two_ff // 2
    capacity = run_experts.capacity
    first = acc is None
    rows_blk = capacity // 2 if capacity % 32 == 0 else capacity
    padded = capacity + WIN
    any_spec = pl.BlockSpec(memory_space=pl.ANY)
    tok_spec = pl.BlockSpec((1, 2, tiles, TILE), lambda e, s: (e, 0, 0, 0))
    once = pl.Buffered(1)
    up_spec = pl.BlockSpec((parts, 1, quarter, two_ff), lambda e, s: (0, e, 0, 0))
    down_spec = pl.BlockSpec((parts, 1, quarter, ff), lambda e, s: (0, e, 0, 0))
    up_once = pl.BlockSpec((parts, 1, quarter, two_ff), lambda e, s: (0, e, 0, 0), pipeline_mode=once)
    down_once = pl.BlockSpec((parts, 1, quarter, ff), lambda e, s: (0, e, 0, 0), pipeline_mode=once)
    in_specs = [tok_spec, tok_spec] + [any_spec] * 4 + [up_spec, down_spec]
    args = [starts, pos, gate, xa, xb, ya, yb, w_up, w_down]
    if not first:
        in_specs += [up_once, down_once]
        args += list(acc)
    flops = n_exp * 2 * (9 * capacity * hidden * ff + 2 * WIN * tok * hidden) * 2
    return pl.pallas_call(
        functools.partial(expert_kernel, first, capacity, rows_blk),
        grid_spec=pltpu.PrefetchScalarGridSpec(
            num_scalar_prefetch=1,
            grid=(n_exp,),
            in_specs=in_specs,
            out_specs=[pl.BlockSpec((1, 2, capacity, hidden), lambda e, s: (e, 0, 0, 0)), tok_spec, up_spec, down_spec],
            scratch_shapes=[
                pltpu.VMEM((2, tok, hidden), BF16),
                pltpu.VMEM((2, tok, hidden), BF16),
                pltpu.VMEM((padded, hidden), BF16),
                pltpu.VMEM((padded, hidden), BF16),
                pltpu.VMEM((padded, 128), F32),
                pltpu.VMEM((padded, 128), F32),
                pltpu.VMEM((capacity, two_ff), BF16),
                pltpu.VMEM((capacity, ff), BF16),
                pltpu.SemaphoreType.DMA((2, 2)),
            ],
        ),
        out_shape=[
            jax.ShapeDtypeStruct((n_exp, 2, capacity, hidden), BF16),
            jax.ShapeDtypeStruct((n_exp, 2, tiles, TILE), F32),
            jax.ShapeDtypeStruct((parts, n_exp, quarter, two_ff), F32),
            jax.ShapeDtypeStruct((parts, n_exp, quarter, ff), F32),
        ],
        compiler_params=pltpu.CompilerParams(dimension_semantics=("arbitrary",), vmem_limit_bytes=66 * 1024 * 1024 - 2 ** 21),
        cost_estimate=pl.CostEstimate(flops=flops, bytes_accessed=90 * 2 ** 20, transcendentals=0),
        name="experts",
    )(*args)


def combine_kernel(n_arr, back_tok, capacity, starts, pos, *rest):
    dxs = rest[:n_arr]
    out = rest[n_arr]
    src = pl.program_id(0)
    lane = lax.broadcasted_iota(jnp.int32, (BACK, TILE), 1)
    per = dxs[0].shape[0]

    def body(i, carry):
        tok0 = pl.multiple_of(jnp.minimum(i * BACK, back_tok), ALIGN)
        total = None
        for e in range(n_arr * per):
            start = pl.multiple_of(starts[src, e, i], ALIGN)
            hit = (lane + start) == pos[0, pl.ds(tok0, BACK), e:e + 1]
            onehot = jnp.where(hit, 1.0, 0.0).astype(BF16)
            term = dot_nn(onehot, dxs[e // per][e % per, 0, pl.ds(start, TILE), :])
            total = term if total is None else total + term
        out[0, pl.ds(tok0, BACK), :] = total.astype(BF16)
        return carry

    lax.fori_loop(0, starts.shape[2], body, 0)


def run_combine(starts, pos, dxs):
    per, _, capacity, hidden = dxs[0].shape
    tok = pos.shape[1]
    n_exp = per * len(dxs)
    return pl.pallas_call(
        functools.partial(combine_kernel, len(dxs), tok - BACK, capacity),
        grid_spec=pltpu.PrefetchScalarGridSpec(
            num_scalar_prefetch=1,
            grid=(2,),
            in_specs=[pl.BlockSpec((1, tok, n_exp), lambda s, st: (s, 0, 0))]
            + [pl.BlockSpec((per, 1, capacity, hidden), lambda s, st: (0, s, 0, 0)) for _ in dxs],
            out_specs=pl.BlockSpec((1, tok, hidden), lambda s, st: (s, 0, 0)),
        ),
        out_shape=jax.ShapeDtypeStruct((2, tok, hidden), BF16),
        compiler_params=pltpu.CompilerParams(dimension_semantics=("arbitrary",), vmem_limit_bytes=48 * 2 ** 20),
        cost_estimate=pl.CostEstimate(flops=2 * n_exp * tok * TILE * hidden * 2, bytes_accessed=20 * 2 ** 20, transcendentals=0),
        name="combine",
    )(starts, pos, *dxs)


def places_of(ids, gates, base, local_experts, capacity):
    n, _, tok = ids.shape
    tiles = tok // TILE
    want = base + jnp.arange(local_experts, dtype=jnp.int32)
    same = ids[:, None, :, :] == want[None, :, None, None]
    gate = jnp.sum(jnp.where(same, gates[:, None, :, :], 0.0), axis=2)
    hit = jnp.any(same, axis=2)
    rows = hit.reshape(n * local_experts * tiles, TILE).astype(BF16)
    upper = (jnp.arange(TILE)[:, None] < jnp.arange(TILE)[None, :]).astype(BF16)
    inside = jnp.dot(rows, upper, preferred_element_type=F32)
    count = jnp.sum(rows.astype(F32), axis=1).reshape(n, local_experts, tiles)
    before = (jnp.arange(tiles)[:, None] < jnp.arange(tiles)[None, :]).astype(F32)
    first = jnp.sum(count[..., :, None] * before, axis=2)
    place = (inside.reshape(n, local_experts, tiles, TILE) + first[..., None]).astype(jnp.int32)
    kept = hit.reshape(n, local_experts, tiles, TILE) & (place < capacity)
    return place, jnp.where(kept, place, -1), gate.reshape(n, local_experts, tiles, TILE)


def solution(mesh):
    ep_size = mesh.shape["ep"]
    tok_spec = P(("fsdp", "ep"), None)
    up_spec = P("ep", "fsdp", None)
    down_spec = P("ep", None, "fsdp")

    def swap(a, mask):
        return lax.ppermute(a, "ep", [(i, i ^ mask) for i in range(ep_size)])

    def add2(a, b):
        return (a.astype(F32) + b.astype(F32)).astype(BF16)

    def per_device(layer_in, out_grad, expert_ids, gate_vals, w_one, w_two, w_three):
        tok, hidden = layer_in.shape
        top_k = expert_ids.shape[1]
        local_experts = w_one.shape[0]
        experts = local_experts * ep_size
        capacity = capacity_of(tok, top_k, experts)
        run_experts.capacity = capacity
        me = lax.axis_index("ep")
        half = local_experts // 2

        x_of = {0: layer_in}
        y_of = {0: out_grad}
        x_of[1], y_of[1] = swap(layer_in, 1), swap(out_grad, 1)
        x_of[2], y_of[2] = swap(layer_in, 2), swap(out_grad, 2)
        x_of[4], y_of[4] = swap(layer_in, 4), swap(out_grad, 4)
        x_of[6], y_of[6] = swap(x_of[2], 4), swap(y_of[4], 2)
        for m in (2, 4, 6):
            x_of[m + 1], y_of[m + 1] = swap(x_of[m], 1), swap(y_of[m], 1)

        up_loc = jnp.concatenate([w_one, w_three], axis=2)
        down_loc = jnp.swapaxes(w_two, 1, 2)
        w_up, w_down = [], []
        for h in range(2):
            w_up.append(lax.all_gather(up_loc[h * half:(h + 1) * half], "fsdp", axis=0))
            w_down.append(lax.all_gather(down_loc[h * half:(h + 1) * half], "fsdp", axis=0))

        ids_t = expert_ids.T
        table = jnp.concatenate([ids_t.astype(F32), gate_vals.T], axis=0)
        tables = lax.all_gather(table, "ep", axis=0)
        tables = jnp.take(tables, me ^ jnp.arange(ep_size, dtype=jnp.int32), axis=0)
        ids = tables[:, :top_k].astype(jnp.int32)
        place, kept, gate = places_of(ids, tables[:, top_k:], me * local_experts, local_experts, capacity)
        first_place = jnp.minimum(place[..., 0], capacity) // ALIGN * ALIGN
        flat_place = place.reshape(ep_size, local_experts, tok)
        n_back = -(-tok // BACK)
        back_at = [min(i * BACK, tok - BACK) for i in range(n_back)]
        back_place = jnp.stack([flat_place[..., t] for t in back_at], axis=-1)
        back_place = jnp.minimum(back_place // ALIGN * ALIGN, capacity - TILE)
        kept_cols = jnp.swapaxes(kept.reshape(ep_size, local_experts, tok), 1, 2)

        def call(k, h, acc):
            m = 2 * k
            es = slice(h * half, (h + 1) * half)
            put = lambda a: jnp.swapaxes(a[m:m + 2, es], 0, 1)
            return run_experts(put(first_place), put(kept), put(gate), x_of[m], x_of[m + 1], y_of[m], y_of[m + 1], w_up[h], w_down[h], acc)

        acc = [None, None]
        dx_of = {}
        dg_of = {}
        sent = {}

        def expert_part(k, h):
            dx, dg, a_up, a_down = call(k, h, acc[h])
            acc[h] = (a_up, a_down)
            dx_of[k, h] = dx
            dg_of[k, h] = dg

        def back_part(k):
            m = 2 * k
            part = run_combine(back_place[m:m + 2], kept_cols[m:m + 2], [dx_of[k, 0], dx_of[k, 1]])
            other = swap(part[1], 1)
            if k == 0:
                sent[0] = (part[0], other)
            else:
                sent[k] = (swap(add2(part[0], other), m),)

        expert_part(0, 0)
        expert_part(0, 1)
        back_part(0)
        expert_part(1, 0)
        expert_part(1, 1)
        back_part(1)
        expert_part(2, 0)
        expert_part(3, 0)
        g_up = [None, None]
        g_down = [None, None]

        def reduce_part(h):
            g_up[h] = lax.psum_scatter(acc[h][0], "fsdp", scatter_dimension=0, tiled=False)
            g_down[h] = lax.psum_scatter(acc[h][1], "fsdp", scatter_dimension=0, tiled=False)

        reduce_part(0)
        expert_part(2, 1)
        back_part(2)
        expert_part(3, 1)
        back_part(3)
        reduce_part(1)

        terms = [t for k in range(ep_size // 2) for t in sent[k]]
        in_grad = functools.reduce(lambda a, b: a + b, [t.astype(F32) for t in terms]).astype(BF16)

        dg = jnp.concatenate([jnp.concatenate([dg_of[k, h] for h in range(2)], axis=0) for k in range(ep_size // 2)], axis=1)
        dg = jnp.swapaxes(dg, 0, 1).reshape(ep_size, local_experts, tok)
        dg = jnp.take(dg, me ^ jnp.arange(ep_size, dtype=jnp.int32), axis=0)
        dg = lax.all_to_all(dg, "ep", 0, 0, tiled=True).reshape(experts, tok)
        pick = ids_t[:, None, :] == jnp.arange(experts, dtype=jnp.int32)[None, :, None]
        gate_out = jnp.sum(jnp.where(pick, dg[None], 0.0), axis=1).T

        up = jnp.concatenate(g_up, axis=0)
        down = jnp.swapaxes(jnp.concatenate(g_down, axis=0), 1, 2)
        ff = w_one.shape[2]
        return in_grad, gate_out, up[:, :, :ff], down, up[:, :, ff:]

    return jax.shard_map(per_device, mesh=mesh, in_specs=(tok_spec, tok_spec, tok_spec, tok_spec, up_spec, down_spec, up_spec), out_specs=(tok_spec, tok_spec, up_spec, down_spec, up_spec), check_vma=False)
```

```python
import functools

import jax
import jax.numpy as jnp
from jax import lax
from jax.experimental import pallas as pl
from jax.experimental.pallas import tpu as pltpu
from jax.sharding import PartitionSpec as P


TILE = 256
ALIGN = 16
WIN = TILE + ALIGN
BACK = TILE - ALIGN
F32 = jnp.float32
BF16 = jnp.bfloat16


def capacity_of(tok_dev, top_k, experts):
    return max(8, ((tok_dev * top_k * 5) // (4 * experts) + 7) // 8 * 8)


def dot_nn(a, b):
    return lax.dot_general(a, b, (((1,), (0,)), ((), ())), preferred_element_type=F32)


def dot_nt(a, b):
    return lax.dot_general(a, b, (((1,), (1,)), ((), ())), preferred_element_type=F32)


def dot_tn(a, b):
    return lax.dot_general(a, b, (((0,), (0,)), ((), ())), preferred_element_type=F32)


def expert_kernel(first, capacity, rows_blk, starts, pos, gate, xa, xb, ya, yb, w_up, w_down, *rest):
    if first:
        dx, dgate, g_up, g_down = rest[:4]
        scratch = rest[4:]
    else:
        acc_up, acc_down, dx, dgate, g_up, g_down = rest[:6]
        scratch = rest[6:]
    xbuf, ybuf, xs, us, gs, dgs, dhs, acts, sems = scratch
    step = pl.program_id(0)
    tok = xbuf.shape[1]
    hidden = xbuf.shape[2]
    ff = acts.shape[1]
    tiles = tok // TILE

    def copies(src):
        x_ref, y_ref = ((xa, ya), (xb, yb))[src]
        return (pltpu.make_async_copy(x_ref, xbuf.at[src], sems.at[src, 0]),
                pltpu.make_async_copy(y_ref, ybuf.at[src], sems.at[src, 1]))

    @pl.when(step == 0)
    def _():
        for src in range(2):
            for cp in copies(src):
                cp.start()

    if first:
        g_up[...] = jnp.zeros_like(g_up)
        g_down[...] = jnp.zeros_like(g_down)
    else:
        g_up[...] = acc_up[...]
        g_down[...] = acc_down[...]

    slot_iota = lax.broadcasted_iota(jnp.int32, (WIN, TILE), 0)

    def source_body(src, carry):
        for n in range(2):
            @pl.when((step == 0) & (src == n))
            def _():
                for cp in copies(n):
                    cp.wait()

        xs[0:capacity, :] = jnp.zeros((capacity, hidden), BF16)
        us[0:capacity, :] = jnp.zeros((capacity, hidden), BF16)
        gs[0:capacity, :] = jnp.zeros((capacity, 128), F32)

        def pick(i, carry):
            start = pl.multiple_of(starts[step, src, i], ALIGN)
            pos_row = pos[0, src, pl.ds(i, 1), :]
            gate_row = gate[0, src, pl.ds(i, 1), :]
            hit = (slot_iota + start) == pos_row
            onehot = jnp.where(hit, 1.0, 0.0).astype(BF16)
            tok0 = pl.multiple_of(i * TILE, TILE)
            for buf, rows in ((xbuf, xs), (ybuf, us)):
                for c in range(0, hidden, 256):
                    got = dot_nn(onehot, buf[src, pl.ds(tok0, TILE), c:c + 256]).astype(BF16)
                    rows[pl.ds(start, ALIGN), c:c + 256] = rows[pl.ds(start, ALIGN), c:c + 256] + got[:ALIGN]
                    rows[pl.ds(start + ALIGN, TILE), c:c + 256] = got[ALIGN:]
            got_gate = jnp.sum(jnp.where(hit, gate_row, 0.0), axis=1, keepdims=True)
            got_gate = jnp.broadcast_to(got_gate, (WIN, 128))
            gs[pl.ds(start, ALIGN), :] = gs[pl.ds(start, ALIGN), :] + got_gate[:ALIGN]
            gs[pl.ds(start + ALIGN, TILE), :] = got_gate[ALIGN:]
            return carry

        lax.fori_loop(0, tiles, pick, 0)

        def rows_body(b, carry):
            r0 = pl.multiple_of(b * rows_blk, rows_blk)
            rows = pl.ds(r0, rows_blk)
            up = w_up[...].reshape(hidden, 2 * ff)
            down = w_down[...].reshape(hidden, ff)
            h = dot_nn(xs[rows, :], up)
            h_one = h[:, :ff]
            h_three = h[:, ff:]
            sig = jax.nn.sigmoid(h_one)
            silu = h_one * sig
            act = (silu * h_three).astype(BF16)
            acts[rows, :] = act
            u = us[rows, :].astype(F32)
            y = dot_nt(act, down)
            dg = jnp.sum(u * y, axis=1, keepdims=True)
            dgs[rows, :] = jnp.broadcast_to(dg, (rows_blk, 128))
            g = (gs[rows, 0:1] * u).astype(BF16)
            us[rows, :] = g
            da = dot_nn(g, down)
            dh_one = (da * h_three * sig * (1.0 + h_one * (1.0 - sig))).astype(BF16)
            dh_three = (da * silu).astype(BF16)
            dhs[rows, 0:ff] = dh_one
            dhs[rows, ff:2 * ff] = dh_three
            dx[0, src, rows, :] = dot_nt(dhs[rows, :], up).astype(BF16)
            return carry

        lax.fori_loop(0, capacity // rows_blk, rows_body, 0)

        quarter = g_up.shape[2]
        for z in range(g_up.shape[0]):
            cols = slice(z * quarter, (z + 1) * quarter)
            g_up[z, 0] += dot_tn(xs[0:capacity, cols], dhs[...])
            g_down[z, 0] += dot_tn(us[0:capacity, cols], acts[...])

        def give(i, carry):
            start = pl.multiple_of(starts[step, src, i], ALIGN)
            hit = (slot_iota + start) == pos[0, src, pl.ds(i, 1), :]
            val = dgs[pl.ds(start, WIN), :]
            val = jnp.concatenate([val, val], axis=1)
            dgate[0, src, pl.ds(i, 1), :] = jnp.sum(jnp.where(hit, val, 0.0), axis=0, keepdims=True)
            return carry

        lax.fori_loop(0, tiles, give, 0)
        return carry

    lax.fori_loop(0, 2, source_body, 0)


def run_experts(starts, pos, gate, xa, xb, ya, yb, w_up, w_down, acc):
    n_exp, _, tiles, _ = pos.shape
    tok, hidden = xa.shape
    parts, _, quarter, two_ff = w_up.shape
    ff = two_ff // 2
    capacity = run_experts.capacity
    first = acc is None
    rows_blk = capacity // 2 if capacity % 32 == 0 else capacity
    padded = capacity + WIN
    any_spec = pl.BlockSpec(memory_space=pl.ANY)
    tok_spec = pl.BlockSpec((1, 2, tiles, TILE), lambda e, s: (e, 0, 0, 0))
    once = pl.Buffered(1)
    up_spec = pl.BlockSpec((parts, 1, quarter, two_ff), lambda e, s: (0, e, 0, 0))
    down_spec = pl.BlockSpec((parts, 1, quarter, ff), lambda e, s: (0, e, 0, 0))
    up_once = pl.BlockSpec((parts, 1, quarter, two_ff), lambda e, s: (0, e, 0, 0), pipeline_mode=once)
    down_once = pl.BlockSpec((parts, 1, quarter, ff), lambda e, s: (0, e, 0, 0), pipeline_mode=once)
    in_specs = [tok_spec, tok_spec] + [any_spec] * 4 + [up_spec, down_spec]
    args = [starts, pos, gate, xa, xb, ya, yb, w_up, w_down]
    if not first:
        in_specs += [up_once, down_once]
        args += list(acc)
    flops = n_exp * 2 * (9 * capacity * hidden * ff + 2 * WIN * tok * hidden) * 2
    return pl.pallas_call(
        functools.partial(expert_kernel, first, capacity, rows_blk),
        grid_spec=pltpu.PrefetchScalarGridSpec(
            num_scalar_prefetch=1,
            grid=(n_exp,),
            in_specs=in_specs,
            out_specs=[pl.BlockSpec((1, 2, capacity, hidden), lambda e, s: (e, 0, 0, 0)), tok_spec, up_spec, down_spec],
            scratch_shapes=[
                pltpu.VMEM((2, tok, hidden), BF16),
                pltpu.VMEM((2, tok, hidden), BF16),
                pltpu.VMEM((padded, hidden), BF16),
                pltpu.VMEM((padded, hidden), BF16),
                pltpu.VMEM((padded, 128), F32),
                pltpu.VMEM((padded, 128), F32),
                pltpu.VMEM((capacity, two_ff), BF16),
                pltpu.VMEM((capacity, ff), BF16),
                pltpu.SemaphoreType.DMA((2, 2)),
            ],
        ),
        out_shape=[
            jax.ShapeDtypeStruct((n_exp, 2, capacity, hidden), BF16),
            jax.ShapeDtypeStruct((n_exp, 2, tiles, TILE), F32),
            jax.ShapeDtypeStruct((parts, n_exp, quarter, two_ff), F32),
            jax.ShapeDtypeStruct((parts, n_exp, quarter, ff), F32),
        ],
        compiler_params=pltpu.CompilerParams(dimension_semantics=("arbitrary",), vmem_limit_bytes=66 * 1024 * 1024 - 2 ** 21),
        cost_estimate=pl.CostEstimate(flops=flops, bytes_accessed=90 * 2 ** 20, transcendentals=0),
        name="experts",
    )(*args)


def combine_kernel(n_arr, back_tok, capacity, starts, pos, *rest):
    dxs = rest[:n_arr]
    mine, theirs = rest[n_arr:]
    src = pl.program_id(0)
    lane = lax.broadcasted_iota(jnp.int32, (BACK, TILE), 1)
    per = dxs[0].shape[0]

    def body(i, carry):
        tok0 = pl.multiple_of(jnp.minimum(i * BACK, back_tok), ALIGN)
        total = None
        for e in range(n_arr * per):
            start = pl.multiple_of(starts[src, e, i], ALIGN)
            hit = (lane + start) == pos[0, pl.ds(tok0, BACK), e:e + 1]
            onehot = jnp.where(hit, 1.0, 0.0).astype(BF16)
            term = dot_nn(onehot, dxs[e // per][e % per, 0, pl.ds(start, TILE), :])
            total = term if total is None else total + term
        total = total.astype(BF16)

        @pl.when(src == 0)
        def _():
            mine[pl.ds(tok0, BACK), :] = total

        @pl.when(src == 1)
        def _():
            theirs[pl.ds(tok0, BACK), :] = total

        return carry

    lax.fori_loop(0, starts.shape[2], body, 0)


def run_combine(starts, pos, dxs):
    per, _, capacity, hidden = dxs[0].shape
    tok = pos.shape[1]
    n_exp = per * len(dxs)
    return pl.pallas_call(
        functools.partial(combine_kernel, len(dxs), tok - BACK, capacity),
        grid_spec=pltpu.PrefetchScalarGridSpec(
            num_scalar_prefetch=1,
            grid=(2,),
            in_specs=[pl.BlockSpec((1, tok, n_exp), lambda s, st: (s, 0, 0))]
            + [pl.BlockSpec((per, 1, capacity, hidden), lambda s, st: (0, s, 0, 0)) for _ in dxs],
            out_specs=[pl.BlockSpec((tok, hidden), lambda s, st: (0, 0))] * 2,
        ),
        out_shape=[jax.ShapeDtypeStruct((tok, hidden), BF16)] * 2,
        compiler_params=pltpu.CompilerParams(dimension_semantics=("arbitrary",), vmem_limit_bytes=48 * 2 ** 20),
        cost_estimate=pl.CostEstimate(flops=2 * n_exp * tok * TILE * hidden * 2, bytes_accessed=20 * 2 ** 20, transcendentals=0),
        name="combine",
    )(starts, pos, *dxs)


def places_of(ids, gates, base, local_experts, capacity):
    n, _, tok = ids.shape
    tiles = tok // TILE
    want = base + jnp.arange(local_experts, dtype=jnp.int32)
    same = ids[:, None, :, :] == want[None, :, None, None]
    gate = jnp.sum(jnp.where(same, gates[:, None, :, :], 0.0), axis=2)
    hit = jnp.any(same, axis=2)
    rows = hit.reshape(n * local_experts * tiles, TILE).astype(BF16)
    upper = (jnp.arange(TILE)[:, None] < jnp.arange(TILE)[None, :]).astype(BF16)
    inside = jnp.dot(rows, upper, preferred_element_type=F32)
    count = jnp.sum(rows.astype(F32), axis=1).reshape(n, local_experts, tiles)
    before = (jnp.arange(tiles)[:, None] < jnp.arange(tiles)[None, :]).astype(F32)
    first = jnp.sum(count[..., :, None] * before, axis=2)
    place = (inside.reshape(n, local_experts, tiles, TILE) + first[..., None]).astype(jnp.int32)
    kept = hit.reshape(n, local_experts, tiles, TILE) & (place < capacity)
    return place, jnp.where(kept, place, -1), gate.reshape(n, local_experts, tiles, TILE)


def solution(mesh):
    ep_size = mesh.shape["ep"]
    tok_spec = P(("fsdp", "ep"), None)
    up_spec = P("ep", "fsdp", None)
    down_spec = P("ep", None, "fsdp")

    def swap(a, mask):
        return lax.ppermute(a, "ep", [(i, i ^ mask) for i in range(ep_size)])

    def add2(a, b):
        return (a.astype(F32) + b.astype(F32)).astype(BF16)

    def per_device(layer_in, out_grad, expert_ids, gate_vals, w_one, w_two, w_three):
        tok, hidden = layer_in.shape
        top_k = expert_ids.shape[1]
        local_experts = w_one.shape[0]
        experts = local_experts * ep_size
        capacity = capacity_of(tok, top_k, experts)
        run_experts.capacity = capacity
        me = lax.axis_index("ep")
        half = local_experts // 2

        ids_t = expert_ids.T
        table = jnp.concatenate([ids_t.astype(F32), gate_vals.T], axis=0)
        tables = jnp.stack([table] + [swap(table, m) for m in range(1, ep_size)], axis=0)
        x_of = {0: layer_in}
        y_of = {0: out_grad}
        x_of[1], y_of[1] = swap(layer_in, 1), swap(out_grad, 1)
        x_out, y_out, tables = lax.optimization_barrier((layer_in, out_grad, tables))
        x_of[2], y_of[2] = swap(x_out, 2), swap(y_out, 2)
        x_of[4], y_of[4] = swap(x_out, 4), swap(y_out, 4)

        def spread():
            got = lax.optimization_barrier((x_of[2], y_of[2], x_of[4], y_of[4]) + last[0])
            x_of[2], y_of[2], x_of[4], y_of[4] = got[:4]
            x_of[6], y_of[6] = swap(x_of[2], 4), swap(y_of[4], 2)
            for m in (2, 4, 6):
                x_of[m + 1], y_of[m + 1] = swap(x_of[m], 1), swap(y_of[m], 1)

        up_loc = jnp.concatenate([w_one, w_three], axis=2)
        down_loc = jnp.swapaxes(w_two, 1, 2)
        w_up, w_down = [], []
        for h in range(2):
            w_up.append(lax.all_gather(up_loc[h * half:(h + 1) * half], "fsdp", axis=0))
            w_down.append(lax.all_gather(down_loc[h * half:(h + 1) * half], "fsdp", axis=0))

        ids = tables[:, :top_k].astype(jnp.int32)
        place, kept, gate = places_of(ids, tables[:, top_k:], me * local_experts, local_experts, capacity)
        first_place = jnp.minimum(place[..., 0], capacity) // ALIGN * ALIGN
        flat_place = place.reshape(ep_size, local_experts, tok)
        n_back = -(-tok // BACK)
        back_at = [min(i * BACK, tok - BACK) for i in range(n_back)]
        back_place = jnp.stack([flat_place[..., t] for t in back_at], axis=-1)
        back_place = jnp.minimum(back_place // ALIGN * ALIGN, capacity - TILE)
        kept_cols = jnp.swapaxes(kept.reshape(ep_size, local_experts, tok), 1, 2)

        acc = [None, None]
        dx_of = {}
        dg_of = {}
        sent = {}
        last = [()]

        def after(a):
            out = lax.optimization_barrier((a,) + tuple(last[0]))
            return out[0]

        def expert_part(k, h):
            m = 2 * k
            es = slice(h * half, (h + 1) * half)
            put = lambda a: jnp.swapaxes(a[m:m + 2, es], 0, 1)
            dx, dg, a_up, a_down = run_experts(after(put(first_place)), put(kept), put(gate), x_of[m], x_of[m + 1], y_of[m], y_of[m + 1], w_up[h], w_down[h], acc[h])
            acc[h] = (a_up, a_down)
            dx_of[k, h] = dx
            dg_of[k, h] = dg
            last[0] = (dg,)

        def combine_part(k):
            m = 2 * k
            mine, theirs = run_combine(after(back_place[m:m + 2]), kept_cols[m:m + 2], [dx_of[k, 0], dx_of[k, 1]])
            last[0] = last[0] + (mine,)
            return mine, swap(theirs, 1)

        def send_part(k, parts):
            total = add2(*lax.optimization_barrier(parts + tuple(last[0]))[:2])
            last[0] = last[0] + (total,)
            sent[k] = (swap(total, 2 * k),)

        expert_part(0, 0)
        spread()
        for k in range(1, 4):
            expert_part(k, 0)
        g_up = [lax.psum_scatter(acc[0][0], "fsdp", scatter_dimension=0, tiled=False)]
        g_down = [lax.psum_scatter(acc[0][1], "fsdp", scatter_dimension=0, tiled=False)]

        expert_part(3, 1)
        parts3 = combine_part(3)
        expert_part(1, 1)
        send_part(3, parts3)
        parts1 = combine_part(1)
        expert_part(2, 1)
        send_part(1, parts1)
        parts2 = combine_part(2)
        send_part(2, parts2)
        expert_part(0, 1)

        a_up, a_down = acc[1]
        n_z = mesh.shape["fsdp"]
        z = lax.axis_index("fsdp")
        take = lambda a, i: lax.dynamic_index_in_dim(a, i, 0, keepdims=False)
        up_1, down_1 = take(a_up, z), take(a_down, z)
        got = []
        for o in (2, 1, 3):
            to = lax.rem(z + o, n_z)
            ring = [(i, (i + o) % n_z) for i in range(n_z)]
            got.append((lax.ppermute(take(a_up, to).astype(BF16), "fsdp", ring), lax.ppermute(take(a_down, to).astype(BF16), "fsdp", ring)))
        sent[0] = combine_part(0)
        g_up.append(functools.reduce(lambda a, b: a + b, [up_1] + [p[0].astype(F32) for p in got]))
        g_down.append(functools.reduce(lambda a, b: a + b, [down_1] + [p[1].astype(F32) for p in got]))

        terms = [t for k in range(ep_size // 2) for t in sent[k]]
        in_grad = functools.reduce(lambda a, b: a + b, [t.astype(F32) for t in terms]).astype(BF16)

        dg = jnp.concatenate([jnp.concatenate([dg_of[k, h] for h in range(2)], axis=0) for k in range(ep_size // 2)], axis=1)
        dg = jnp.swapaxes(dg, 0, 1).reshape(ep_size, local_experts, tok)
        dg = jnp.take(dg, me ^ jnp.arange(ep_size, dtype=jnp.int32), axis=0)
        dg = lax.all_to_all(dg, "ep", 0, 0, tiled=True).reshape(experts, tok)
        pick = ids_t[:, None, :] == jnp.arange(experts, dtype=jnp.int32)[None, :, None]
        gate_out = jnp.sum(jnp.where(pick, dg[None], 0.0), axis=1).T

        up = jnp.concatenate(g_up, axis=0)
        down = jnp.swapaxes(jnp.concatenate(g_down, axis=0), 1, 2)
        ff = w_one.shape[2]
        return in_grad, gate_out, up[:, :, :ff], down, up[:, :, ff:]

    return jax.shard_map(per_device, mesh=mesh, in_specs=(tok_spec, tok_spec, tok_spec, tok_spec, up_spec, down_spec, up_spec), out_specs=(tok_spec, tok_spec, up_spec, down_spec, up_spec), check_vma=False)
```

```python
import functools

import jax
import jax.numpy as jnp
from jax import lax
from jax.experimental import pallas as pl
from jax.experimental.pallas import tpu as pltpu
from jax.sharding import PartitionSpec as P


TILE = 256
ALIGN = 16
WIN = TILE + ALIGN
BACK = TILE - ALIGN
F32 = jnp.float32
BF16 = jnp.bfloat16


def capacity_of(tok_dev, top_k, experts):
    return max(8, ((tok_dev * top_k * 5) // (4 * experts) + 7) // 8 * 8)


def dot_nn(a, b):
    return lax.dot_general(a, b, (((1,), (0,)), ((), ())), preferred_element_type=F32)


def dot_nt(a, b):
    return lax.dot_general(a, b, (((1,), (1,)), ((), ())), preferred_element_type=F32)


def dot_tn(a, b):
    return lax.dot_general(a, b, (((0,), (0,)), ((), ())), preferred_element_type=F32)


def expert_kernel(first, capacity, rows_blk, starts, pos, gate, xa, xb, ya, yb, w_up, w_down, *rest):
    if first:
        dx, dgate, g_up, g_down = rest[:4]
        scratch = rest[4:]
    else:
        acc_up, acc_down, dx, dgate, g_up, g_down = rest[:6]
        scratch = rest[6:]
    xbuf, ybuf, xs, us, gs, dgs, dhs, acts, sems = scratch
    step = pl.program_id(0)
    tok = xbuf.shape[1]
    hidden = xbuf.shape[2]
    ff = acts.shape[1]
    tiles = tok // TILE

    def copies(src):
        x_ref, y_ref = ((xa, ya), (xb, yb))[src]
        return (pltpu.make_async_copy(x_ref, xbuf.at[src], sems.at[src, 0]),
                pltpu.make_async_copy(y_ref, ybuf.at[src], sems.at[src, 1]))

    @pl.when(step == 0)
    def _():
        for src in range(2):
            for cp in copies(src):
                cp.start()

    if first:
        g_up[...] = jnp.zeros_like(g_up)
        g_down[...] = jnp.zeros_like(g_down)
    else:
        g_up[...] = acc_up[...]
        g_down[...] = acc_down[...]

    slot_iota = lax.broadcasted_iota(jnp.int32, (WIN, TILE), 0)

    def source_body(src, carry):
        for n in range(2):
            @pl.when((step == 0) & (src == n))
            def _():
                for cp in copies(n):
                    cp.wait()

        xs[0:capacity, :] = jnp.zeros((capacity, hidden), BF16)
        us[0:capacity, :] = jnp.zeros((capacity, hidden), BF16)
        gs[0:capacity, :] = jnp.zeros((capacity, 128), F32)

        def pick(i, carry):
            start = pl.multiple_of(starts[step, src, i], ALIGN)
            pos_row = pos[0, src, pl.ds(i, 1), :]
            gate_row = gate[0, src, pl.ds(i, 1), :]
            hit = (slot_iota + start) == pos_row
            onehot = jnp.where(hit, 1.0, 0.0).astype(BF16)
            tok0 = pl.multiple_of(i * TILE, TILE)
            for buf, rows in ((xbuf, xs), (ybuf, us)):
                for c in range(0, hidden, 256):
                    got = dot_nn(onehot, buf[src, pl.ds(tok0, TILE), c:c + 256]).astype(BF16)
                    rows[pl.ds(start, ALIGN), c:c + 256] = rows[pl.ds(start, ALIGN), c:c + 256] + got[:ALIGN]
                    rows[pl.ds(start + ALIGN, TILE), c:c + 256] = got[ALIGN:]
            got_gate = jnp.sum(jnp.where(hit, gate_row, 0.0), axis=1, keepdims=True)
            got_gate = jnp.broadcast_to(got_gate, (WIN, 128))
            gs[pl.ds(start, ALIGN), :] = gs[pl.ds(start, ALIGN), :] + got_gate[:ALIGN]
            gs[pl.ds(start + ALIGN, TILE), :] = got_gate[ALIGN:]
            return carry

        lax.fori_loop(0, tiles, pick, 0)

        def rows_body(b, carry):
            r0 = pl.multiple_of(b * rows_blk, rows_blk)
            rows = pl.ds(r0, rows_blk)
            up = w_up[...].reshape(hidden, 2 * ff)
            down = w_down[...].reshape(hidden, ff)
            h = dot_nn(xs[rows, :], up)
            h_one = h[:, :ff]
            h_three = h[:, ff:]
            sig = jax.nn.sigmoid(h_one)
            silu = h_one * sig
            act = (silu * h_three).astype(BF16)
            acts[rows, :] = act
            u = us[rows, :].astype(F32)
            y = dot_nt(act, down)
            dg = jnp.sum(u * y, axis=1, keepdims=True)
            dgs[rows, :] = jnp.broadcast_to(dg, (rows_blk, 128))
            g = (gs[rows, 0:1] * u).astype(BF16)
            us[rows, :] = g
            da = dot_nn(g, down)
            dh_one = (da * h_three * sig * (1.0 + h_one * (1.0 - sig))).astype(BF16)
            dh_three = (da * silu).astype(BF16)
            dhs[rows, 0:ff] = dh_one
            dhs[rows, ff:2 * ff] = dh_three
            dx[0, src, rows, :] = dot_nt(dhs[rows, :], up).astype(BF16)
            return carry

        lax.fori_loop(0, capacity // rows_blk, rows_body, 0)

        quarter = g_up.shape[2]
        for z in range(g_up.shape[0]):
            cols = slice(z * quarter, (z + 1) * quarter)
            g_up[z, 0] += dot_tn(xs[0:capacity, cols], dhs[...])
            g_down[z, 0] += dot_tn(us[0:capacity, cols], acts[...])

        def give(i, carry):
            start = pl.multiple_of(starts[step, src, i], ALIGN)
            hit = (slot_iota + start) == pos[0, src, pl.ds(i, 1), :]
            val = dgs[pl.ds(start, WIN), :]
            val = jnp.concatenate([val, val], axis=1)
            dgate[0, src, pl.ds(i, 1), :] = jnp.sum(jnp.where(hit, val, 0.0), axis=0, keepdims=True)
            return carry

        lax.fori_loop(0, tiles, give, 0)
        return carry

    lax.fori_loop(0, 2, source_body, 0)


def run_experts(starts, pos, gate, xa, xb, ya, yb, w_up, w_down, acc):
    n_exp, _, tiles, _ = pos.shape
    tok, hidden = xa.shape
    parts, _, quarter, two_ff = w_up.shape
    ff = two_ff // 2
    capacity = run_experts.capacity
    first = acc is None
    rows_blk = capacity // 2 if capacity % 32 == 0 else capacity
    padded = capacity + WIN
    any_spec = pl.BlockSpec(memory_space=pl.ANY)
    tok_spec = pl.BlockSpec((1, 2, tiles, TILE), lambda e, s: (e, 0, 0, 0))
    once = pl.Buffered(1)
    up_spec = pl.BlockSpec((parts, 1, quarter, two_ff), lambda e, s: (0, e, 0, 0))
    down_spec = pl.BlockSpec((parts, 1, quarter, ff), lambda e, s: (0, e, 0, 0))
    up_once = pl.BlockSpec((parts, 1, quarter, two_ff), lambda e, s: (0, e, 0, 0), pipeline_mode=once)
    down_once = pl.BlockSpec((parts, 1, quarter, ff), lambda e, s: (0, e, 0, 0), pipeline_mode=once)
    in_specs = [tok_spec, tok_spec] + [any_spec] * 4 + [up_spec, down_spec]
    args = [starts, pos, gate, xa, xb, ya, yb, w_up, w_down]
    if not first:
        in_specs += [up_once, down_once]
        args += list(acc)
    flops = n_exp * 2 * (9 * capacity * hidden * ff + 2 * WIN * tok * hidden) * 2
    return pl.pallas_call(
        functools.partial(expert_kernel, first, capacity, rows_blk),
        grid_spec=pltpu.PrefetchScalarGridSpec(
            num_scalar_prefetch=1,
            grid=(n_exp,),
            in_specs=in_specs,
            out_specs=[pl.BlockSpec((1, 2, capacity, hidden), lambda e, s: (e, 0, 0, 0)), tok_spec, up_spec, down_spec],
            scratch_shapes=[
                pltpu.VMEM((2, tok, hidden), BF16),
                pltpu.VMEM((2, tok, hidden), BF16),
                pltpu.VMEM((padded, hidden), BF16),
                pltpu.VMEM((padded, hidden), BF16),
                pltpu.VMEM((padded, 128), F32),
                pltpu.VMEM((padded, 128), F32),
                pltpu.VMEM((capacity, two_ff), BF16),
                pltpu.VMEM((capacity, ff), BF16),
                pltpu.SemaphoreType.DMA((2, 2)),
            ],
        ),
        out_shape=[
            jax.ShapeDtypeStruct((n_exp, 2, capacity, hidden), BF16),
            jax.ShapeDtypeStruct((n_exp, 2, tiles, TILE), F32),
            jax.ShapeDtypeStruct((parts, n_exp, quarter, two_ff), F32),
            jax.ShapeDtypeStruct((parts, n_exp, quarter, ff), F32),
        ],
        compiler_params=pltpu.CompilerParams(dimension_semantics=("arbitrary",), vmem_limit_bytes=66 * 1024 * 1024 - 2 ** 21),
        cost_estimate=pl.CostEstimate(flops=flops, bytes_accessed=90 * 2 ** 20, transcendentals=0),
        name="experts",
    )(*args)


def combine_kernel(n_arr, back_tok, capacity, starts, pos, *rest):
    dxs = rest[:n_arr]
    mine, theirs = rest[n_arr:]
    src = pl.program_id(0)
    lane = lax.broadcasted_iota(jnp.int32, (BACK, TILE), 1)
    per = dxs[0].shape[0]

    def body(i, carry):
        tok0 = pl.multiple_of(jnp.minimum(i * BACK, back_tok), ALIGN)
        total = None
        for e in range(n_arr * per):
            start = pl.multiple_of(starts[src, e, i], ALIGN)
            hit = (lane + start) == pos[0, pl.ds(tok0, BACK), e:e + 1]
            onehot = jnp.where(hit, 1.0, 0.0).astype(BF16)
            term = dot_nn(onehot, dxs[e // per][e % per, 0, pl.ds(start, TILE), :])
            total = term if total is None else total + term
        total = total.astype(BF16)

        @pl.when(src == 0)
        def _():
            mine[pl.ds(tok0, BACK), :] = total

        @pl.when(src == 1)
        def _():
            theirs[pl.ds(tok0, BACK), :] = total

        return carry

    lax.fori_loop(0, starts.shape[2], body, 0)


def run_combine(starts, pos, dxs):
    per, _, capacity, hidden = dxs[0].shape
    tok = pos.shape[1]
    n_exp = per * len(dxs)
    return pl.pallas_call(
        functools.partial(combine_kernel, len(dxs), tok - BACK, capacity),
        grid_spec=pltpu.PrefetchScalarGridSpec(
            num_scalar_prefetch=1,
            grid=(2,),
            in_specs=[pl.BlockSpec((1, tok, n_exp), lambda s, st: (s, 0, 0))]
            + [pl.BlockSpec((per, 1, capacity, hidden), lambda s, st: (0, s, 0, 0)) for _ in dxs],
            out_specs=[pl.BlockSpec((tok, hidden), lambda s, st: (0, 0))] * 2,
        ),
        out_shape=[jax.ShapeDtypeStruct((tok, hidden), BF16)] * 2,
        compiler_params=pltpu.CompilerParams(dimension_semantics=("arbitrary",), vmem_limit_bytes=48 * 2 ** 20),
        cost_estimate=pl.CostEstimate(flops=2 * n_exp * tok * TILE * hidden * 2, bytes_accessed=20 * 2 ** 20, transcendentals=0),
        name="combine",
    )(starts, pos, *dxs)


def places_of(ids, gates, base, local_experts, capacity):
    n, _, tok = ids.shape
    tiles = tok // TILE
    want = base + jnp.arange(local_experts, dtype=jnp.int32)
    same = ids[:, None, :, :] == want[None, :, None, None]
    gate = jnp.sum(jnp.where(same, gates[:, None, :, :], 0.0), axis=2)
    hit = jnp.any(same, axis=2)
    rows = hit.reshape(n * local_experts * tiles, TILE).astype(BF16)
    upper = (jnp.arange(TILE)[:, None] < jnp.arange(TILE)[None, :]).astype(BF16)
    inside = jnp.dot(rows, upper, preferred_element_type=F32)
    count = jnp.sum(rows.astype(F32), axis=1).reshape(n, local_experts, tiles)
    before = (jnp.arange(tiles)[:, None] < jnp.arange(tiles)[None, :]).astype(F32)
    first = jnp.sum(count[..., :, None] * before, axis=2)
    place = (inside.reshape(n, local_experts, tiles, TILE) + first[..., None]).astype(jnp.int32)
    kept = hit.reshape(n, local_experts, tiles, TILE) & (place < capacity)
    return place, jnp.where(kept, place, -1), gate.reshape(n, local_experts, tiles, TILE)


def solution(mesh):
    ep_size = mesh.shape["ep"]
    tok_spec = P(("fsdp", "ep"), None)
    up_spec = P("ep", "fsdp", None)
    down_spec = P("ep", None, "fsdp")

    def swap(a, mask):
        return lax.ppermute(a, "ep", [(i, i ^ mask) for i in range(ep_size)])

    def add2(a, b):
        return (a.astype(F32) + b.astype(F32)).astype(BF16)

    def per_device(layer_in, out_grad, expert_ids, gate_vals, w_one, w_two, w_three):
        tok, hidden = layer_in.shape
        top_k = expert_ids.shape[1]
        local_experts = w_one.shape[0]
        experts = local_experts * ep_size
        capacity = capacity_of(tok, top_k, experts)
        run_experts.capacity = capacity
        me = lax.axis_index("ep")
        half = local_experts // 2

        ids_t = expert_ids.T
        table = jnp.concatenate([ids_t.astype(F32), gate_vals.T], axis=0)
        tables = jnp.stack([table] + [swap(table, m) for m in range(1, ep_size)], axis=0)
        x_of = {0: layer_in}
        y_of = {0: out_grad}
        x_of[1], y_of[1] = swap(layer_in, 1), swap(out_grad, 1)
        x_out, y_out, tables = lax.optimization_barrier((layer_in, out_grad, tables))
        x_of[2], y_of[2] = swap(x_out, 2), swap(y_out, 2)
        x_of[4], y_of[4] = swap(x_out, 4), swap(y_out, 4)

        x_of[6], x_of[3], x_of[5] = swap(x_of[2], 4), swap(x_of[2], 1), swap(x_of[4], 1)

        def spread():
            y_of[2], y_of[4] = lax.optimization_barrier((y_of[2], y_of[4]) + last[0])[:2]
            y_of[3], y_of[5], y_of[6] = swap(y_of[2], 1), swap(y_of[4], 1), swap(y_of[4], 2)

        def spread_diagonal():
            x_of[6], y_of[6] = lax.optimization_barrier((x_of[6], y_of[6]) + last[0])[:2]
            x_of[7], y_of[7] = swap(x_of[6], 1), swap(y_of[6], 1)

        up_loc = jnp.concatenate([w_one, w_three], axis=2)
        down_loc = jnp.swapaxes(w_two, 1, 2)
        w_up, w_down = [], []
        for h in range(2):
            w_up.append(lax.all_gather(up_loc[h * half:(h + 1) * half], "fsdp", axis=0))
            w_down.append(lax.all_gather(down_loc[h * half:(h + 1) * half], "fsdp", axis=0))

        ids = tables[:, :top_k].astype(jnp.int32)
        place, kept, gate = places_of(ids, tables[:, top_k:], me * local_experts, local_experts, capacity)
        first_place = jnp.minimum(place[..., 0], capacity) // ALIGN * ALIGN
        flat_place = place.reshape(ep_size, local_experts, tok)
        n_back = -(-tok // BACK)
        back_at = [min(i * BACK, tok - BACK) for i in range(n_back)]
        back_place = jnp.stack([flat_place[..., t] for t in back_at], axis=-1)
        back_place = jnp.minimum(back_place // ALIGN * ALIGN, capacity - TILE)
        kept_cols = jnp.swapaxes(kept.reshape(ep_size, local_experts, tok), 1, 2)

        acc = [None, None]
        dx_of = {}
        dg_of = {}
        sent = {}
        last = [()]

        def after(a):
            out = lax.optimization_barrier((a,) + tuple(last[0]))
            return out[0]

        def expert_part(k, h):
            m = 2 * k
            es = slice(h * half, (h + 1) * half)
            put = lambda a: jnp.swapaxes(a[m:m + 2, es], 0, 1)
            dx, dg, a_up, a_down = run_experts(after(put(first_place)), put(kept), put(gate), x_of[m], x_of[m + 1], y_of[m], y_of[m + 1], w_up[h], w_down[h], acc[h])
            acc[h] = (a_up, a_down)
            dx_of[k, h] = dx
            dg_of[k, h] = dg
            last[0] = (dg,)

        def combine_part(k):
            m = 2 * k
            mine, theirs = run_combine(after(back_place[m:m + 2]), kept_cols[m:m + 2], [dx_of[k, 0], dx_of[k, 1]])
            last[0] = last[0] + (mine,)
            return mine, swap(theirs, 1)

        def send_part(k, parts):
            total = add2(*lax.optimization_barrier(parts + tuple(last[0]))[:2])
            last[0] = last[0] + (total,)
            sent[k] = (swap(total, 2 * k),)

        expert_part(0, 0)
        spread()
        expert_part(1, 0)
        spread_diagonal()
        expert_part(2, 0)
        expert_part(3, 0)
        g_up = [lax.psum_scatter(acc[0][0], "fsdp", scatter_dimension=0, tiled=False)]
        g_down = [lax.psum_scatter(acc[0][1], "fsdp", scatter_dimension=0, tiled=False)]

        expert_part(3, 1)
        parts3 = combine_part(3)
        expert_part(1, 1)
        send_part(3, parts3)
        parts1 = combine_part(1)
        expert_part(2, 1)
        send_part(1, parts1)
        parts2 = combine_part(2)
        send_part(2, parts2)
        expert_part(0, 1)

        a_up, a_down = acc[1]
        n_z = mesh.shape["fsdp"]
        z = lax.axis_index("fsdp")
        take = lambda a, i: lax.dynamic_index_in_dim(a, i, 0, keepdims=False)
        up_1, down_1 = take(a_up, z), take(a_down, z)
        got = []
        for o in (2, 1, 3):
            to = lax.rem(z + o, n_z)
            ring = [(i, (i + o) % n_z) for i in range(n_z)]
            away = (take(a_up, to).astype(BF16), take(a_down, to).astype(BF16))
            last[0] = last[0] + away
            got.append([lax.ppermute(a, "fsdp", ring) for a in away])
        sent[0] = combine_part(0)
        g_up.append(functools.reduce(lambda a, b: a + b, [up_1] + [p[0].astype(F32) for p in got]))
        g_down.append(functools.reduce(lambda a, b: a + b, [down_1] + [p[1].astype(F32) for p in got]))

        terms = [t for k in range(ep_size // 2) for t in sent[k]]
        in_grad = functools.reduce(lambda a, b: a + b, [t.astype(F32) for t in terms]).astype(BF16)

        dg = jnp.concatenate([jnp.concatenate([dg_of[k, h] for h in range(2)], axis=0) for k in range(ep_size // 2)], axis=1)
        dg = jnp.swapaxes(dg, 0, 1).reshape(ep_size, local_experts, tok)
        dg = jnp.take(dg, me ^ jnp.arange(ep_size, dtype=jnp.int32), axis=0)
        dg = lax.all_to_all(dg, "ep", 0, 0, tiled=True).reshape(experts, tok)
        pick = ids_t[:, None, :] == jnp.arange(experts, dtype=jnp.int32)[None, :, None]
        gate_out = jnp.sum(jnp.where(pick, dg[None], 0.0), axis=1).T

        up = jnp.concatenate(g_up, axis=0)
        down = jnp.swapaxes(jnp.concatenate(g_down, axis=0), 1, 2)
        ff = w_one.shape[2]
        return in_grad, gate_out, up[:, :, :ff], down, up[:, :, ff:]

    return jax.shard_map(per_device, mesh=mesh, in_specs=(tok_spec, tok_spec, tok_spec, tok_spec, up_spec, down_spec, up_spec), out_specs=(tok_spec, tok_spec, up_spec, down_spec, up_spec), check_vma=False)
```
